32 devices in a mesh: tm: 8 (over y, x, core), sr: 4 (over z).
Axes of the slice: x: 2, y: 2, z: 4, core: 2. Of those that a mesh axis runs over, the one named last changes fastest.
Arguments:
- observations: bfloat16 [1024, 65536], P(None, ('sr', 'tm')), may hold values from -6 to 6
- loadings: float32 [65536, 128], P(('sr', 'tm')), may hold values from -0.0007324219 to 0.0007324219
- noise_precision: float32 [65536], P(('sr', 'tm')), may hold values from 0.5 to 4
- transition: float32 [128, 128], replicated, may hold values from -1 to 1, as said below
- filter_cov: float32 [128, 128], replicated, may hold values from -1 to 1, as said below
- smoother_gain: float32 [128, 128], replicated, may hold values from -1 to 1, as said below
- smoothed_cov: float32 [128, 128], replicated, may hold values from -1 to 1, as said below
Outputs:
- smoothed_factors: float32 [1024, 128], P('tm')
- new_loadings: float32 [65536, 128], P(('sr', 'tm'))
- new_transition: float32 [128, 128], replicated
The draws below stay inside these ranges and needn't reach their ends.
Inputs may be any that keep to these rules, and one draw needn't show every extreme that they name: `transition`: the spectral radius is below one. `filter_cov`: symmetric positive definite. `smoother_gain`: the spectral radius is below one. `smoothed_cov`: symmetric positive definite.
All inputs are finite; a program needn't handle non-finite values.
Results may differ from the reference program's by a relative error of at most 0.00175.
The reference program's roundings to bfloat16 on the way (of `scaled` and `factors_b`) count: a program that leaves them out, or rounds other values in their place, can miss the bound.
Values may be sent and summed in bfloat16 or wider, within the bound.
A program may use at most 64 MiB of HBM per device.

```python
import math
import jax
import jax.numpy as jnp
from jax import lax

SERIES = 65536
FACTORS = 128
TIME = 1024


def modal_parts(key):
    base = jax.random.fold_in(key, 4711)
    subkeys = jax.random.split(base, 10)
    normal_basis = jax.random.normal(subkeys[0], (FACTORS, FACTORS), jnp.float32)
    basis, unused = jnp.linalg.qr(normal_basis)
    slowness = jax.random.randint(subkeys[1], (FACTORS // 2,), 0, 2) > 0
    return (basis, slowness, subkeys)


def rotation_blocks(radius, angle):
    evens = jnp.arange(0, FACTORS, 2)
    cosine = radius * jnp.cos(angle)
    sine = radius * jnp.sin(angle)
    matrix = jnp.zeros((FACTORS, FACTORS), jnp.float32)
    matrix = matrix.at[evens, evens].set(cosine).at[evens, evens + 1].set(-sine)
    matrix = matrix.at[evens + 1, evens].set(sine).at[evens + 1, evens + 1].set(cosine)
    return matrix


def turning(basis, slowness, first_key, second_key, angle_key):
    half = FACTORS // 2
    slow_radius = jnp.exp(-jax.random.uniform(first_key, (half,), jnp.float32, 0.1, 0.6) / TIME)
    fast_radius = jnp.exp(-1.0 / jax.random.uniform(second_key, (half,), jnp.float32, 30.0, 50.0))
    radius = jnp.where(slowness, slow_radius, fast_radius)
    angle = jax.random.uniform(angle_key, (half,), jnp.float32, 0.3, 2.8)
    inner = rotation_blocks(radius, angle)
    return jnp.dot(jnp.dot(basis, inner, precision=lax.Precision.HIGHEST), basis.T, precision=lax.Precision.HIGHEST)


def draw_transition(key, part):
    basis, slowness, subkeys = modal_parts(key)
    return turning(basis, slowness, subkeys[2], subkeys[3], subkeys[4])


def draw_smoother_gain(key, part):
    basis, slowness, subkeys = modal_parts(key)
    return turning(basis, slowness, subkeys[5], subkeys[6], subkeys[7])


def draw_filter_cov(key, part):
    basis, slowness, subkeys = modal_parts(key)
    values = jnp.exp(jax.random.uniform(subkeys[8], (FACTORS,), jnp.float32, jnp.log(0.2), 0.0))
    return jnp.dot(basis * values[None, :], basis.T, precision=lax.Precision.HIGHEST)


def draw_smoothed_cov(key, part):
    basis, slowness, subkeys = modal_parts(key)
    values = jax.random.uniform(subkeys[9], (FACTORS,), jnp.float32, 0.3, 1.0)
    return jnp.dot(basis * values[None, :], basis.T, precision=lax.Precision.HIGHEST)


def block_levels(own_key, extent, shards, low, top_value):
    loudness = 1.0
    for axis_at, shards_of in shards:
        draws = jax.random.uniform(jax.random.fold_in(jax.random.fold_in(own_key, 6), axis_at), (shards_of,), jnp.float32, low / len(shards), top_value / len(shards))
        loudness = loudness * jnp.repeat(jnp.exp(draws), extent[axis_at] // shards_of).reshape((-1,) + (1,) * (len(extent) - 1 - axis_at))
    return loudness


def normal_values(key, dims, width, bound, cuts=(), dtype=jnp.bfloat16):
    level = block_levels(key, dims, cuts, -0.22, 0.18) if cuts else 1.0
    values = jax.random.normal(key, dims, jnp.float32) * width * level
    return jnp.minimum(jnp.maximum(values, -bound), bound).astype(dtype)


def setup_inputs(seed: int = 0) -> dict:
    splits = jax.random.split(jax.random.key(seed), 8)
    observations = normal_values(splits[0], (TIME, SERIES), 1.0, 6.0, ((1, 32),))
    loadings = normal_values(splits[1], (SERIES, FACTORS), (SERIES * TIME) ** -0.5, 0.0007324219, ((0, 32),), jnp.float32)
    noise_precision = jnp.clip(jnp.exp(math.log(4.0) - 2.0794415 * jax.random.uniform(splits[2], (SERIES,), jnp.float32) ** block_levels(splits[2], (SERIES,), ((0, 32),), -0.2, 0.2)), 0.5, 4.0)
    transition = draw_transition(jax.random.fold_in(splits[7], 71), 0)
    filter_cov = draw_filter_cov(jax.random.fold_in(splits[7], 71), 0)
    smoother_gain = draw_smoother_gain(jax.random.fold_in(splits[7], 71), 0)
    smoothed_cov = draw_smoothed_cov(jax.random.fold_in(splits[7], 71), 0)
    return dict(observations=observations, loadings=loadings, noise_precision=noise_precision, transition=transition, filter_cov=filter_cov, smoother_gain=smoother_gain, smoothed_cov=smoothed_cov)


precise = lax.Precision.HIGHEST

def dot_high(left, right):
    return jnp.dot(left.astype(jnp.float32), right.astype(jnp.float32), precision=precise, preferred_element_type=jnp.float32)

def reference(observations, loadings, noise_precision, transition, filter_cov, smoother_gain, smoothed_cov):
    scaled = (noise_precision[:, None] * loadings).astype(jnp.bfloat16)
    proj = jnp.dot(observations.astype(jnp.float32), scaled.astype(jnp.float32), preferred_element_type=jnp.float32)
    info = dot_high(loadings.T, noise_precision[:, None] * loadings)
    closed = transition - dot_high(filter_cov, dot_high(info, transition))
    inputs = dot_high(proj, filter_cov.T)

    def forward(state, drive):
        following = dot_high(closed, state) + drive
        return (following, following)
    unused, filtered = lax.scan(forward, jnp.zeros((FACTORS,), jnp.float32), inputs)
    coupled = dot_high(smoother_gain, transition)
    back = filtered - dot_high(filtered, coupled.T)
    back = back.at[TIME - 1].set(filtered[TIME - 1])

    def backward(state, drive):
        following = dot_high(smoother_gain, state) + drive
        return (following, following)
    unused, smoothed = lax.scan(backward, jnp.zeros((FACTORS,), jnp.float32), back, reverse=True)
    factors_b = smoothed.astype(jnp.bfloat16)
    cross = jnp.einsum('ts,tk->sk', observations.astype(jnp.float32), factors_b.astype(jnp.float32), preferred_element_type=jnp.float32)
    total = dot_high(smoothed.T, smoothed) + TIME * smoothed_cov
    previous = dot_high(smoothed[:-1].T, smoothed[:-1]) + (TIME - 1) * smoothed_cov
    lagged = dot_high(smoothed[1:].T, smoothed[:-1]) + (TIME - 1) * dot_high(smoothed_cov, smoother_gain.T)
    total_factor = jnp.linalg.cholesky(total)
    new_loadings = jax.scipy.linalg.cho_solve((total_factor, True), cross.T).T
    previous_factor = jnp.linalg.cholesky(previous)
    new_transition = jax.scipy.linalg.cho_solve((previous_factor, True), lagged.T).T
    return (smoothed, new_loadings, new_transition)
```

```python
import functools
import jax
import jax.numpy as jnp
from jax import lax
from jax.experimental import pallas as pl
from jax.experimental.pallas import tpu as pltpu
from jax.sharding import PartitionSpec as P

precise = lax.Precision.HIGHEST
MESH = pl.DeviceIdType.MESH
SLABS = 8


def dot_high(left, right):
    return jnp.dot(left, right, precision=precise, preferred_element_type=jnp.float32)


def dot_first(left, right):
    return lax.dot_general(
        left, right, (((0,), (0,)), ((), ())), precision=precise, preferred_element_type=jnp.float32
    )


def halves(value):
    high = value.astype(jnp.bfloat16)
    low = (value - high.astype(jnp.float32)).astype(jnp.bfloat16)
    return high, low


def weights(matrix):
    high, low = halves(matrix)
    side = jnp.concatenate([high, low], axis=1)
    return jnp.concatenate([side, side], axis=0)


def times(value, doubled):
    high, low = halves(value)
    width = value.shape[1]
    out = jnp.dot(
        jnp.concatenate([high, low], axis=1), doubled, preferred_element_type=jnp.float32
    )
    return out[:, :width] + out[:, width:]


def reduce_kernel(
    chips, planes, part, out, pair_in, mine, chip_in, plane_in,
    pair_send, pair_recv, chip_send, chip_recv, plane_send, plane_recv,
    back_send, back_recv, last_send, last_recv,
):
    tm = lax.axis_index("tm")
    sr = lax.axis_index("sr")
    core = lax.rem(tm, 2)
    chip = tm // 2
    other = 1 - core
    partner = (2 * chip + other, sr)

    def chip_at(step):
        return lax.rem(chip + step, chips)

    def plane_at(step):
        return lax.rem(sr + step, planes)

    barrier = pltpu.get_barrier_semaphore()
    pl.semaphore_signal(barrier, inc=1, device_id=partner, device_id_type=MESH)
    for step in range(1, chips):
        pl.semaphore_signal(
            barrier, inc=1, device_id=(2 * chip_at(step) + core, sr), device_id_type=MESH
        )
    for step in range(1, planes):
        pl.semaphore_signal(barrier, inc=1, device_id=(tm, plane_at(step)), device_id_type=MESH)
    pl.semaphore_wait(barrier, 1 + chips - 1 + planes - 1)

    order = list(range(1, chips)) + [0]
    pairs = {}
    for step in order:
        target = chip_at(step)
        pairs[step] = pltpu.make_async_remote_copy(
            src_ref=part.at[other, target],
            dst_ref=pair_in.at[step],
            send_sem=pair_send.at[step],
            recv_sem=pair_recv.at[step],
            device_id=partner,
            device_id_type=MESH,
        )
        pairs[step].start()
    across = {}
    for step in order:
        pairs[step].wait_recv()
        mine[step] = part[core, chip_at(step)] + pair_in[step]
        if step > 0:
            across[step] = pltpu.make_async_remote_copy(
                src_ref=mine.at[step],
                dst_ref=chip_in.at[step],
                send_sem=chip_send.at[step],
                recv_sem=chip_recv.at[step],
                device_id=(2 * chip_at(step) + core, sr),
                device_id_type=MESH,
            )
            across[step].start()
    total = mine[0]
    for step in range(1, chips):
        across[step].wait_recv()
        total = total + chip_in[step]
    plane_in[sr] = total
    along = {}
    for step in range(1, planes):
        along[step] = pltpu.make_async_remote_copy(
            src_ref=plane_in.at[sr],
            dst_ref=plane_in.at[sr],
            send_sem=plane_send.at[step],
            recv_sem=plane_recv.at[step],
            device_id=(tm, plane_at(step)),
            device_id_type=MESH,
        )
        along[step].start()
    for step in range(1, planes):
        along[step].wait_recv()
    whole = plane_in[0]
    for plane in range(1, planes):
        whole = whole + plane_in[plane]
    out[core, chip] = whole
    back = {}
    for step in range(1, chips):
        back[step] = pltpu.make_async_remote_copy(
            src_ref=out.at[core, chip],
            dst_ref=out.at[core, chip],
            send_sem=back_send.at[step],
            recv_sem=back_recv.at[step],
            device_id=(2 * chip_at(step) + core, sr),
            device_id_type=MESH,
        )
        back[step].start()
    last = {}
    for step in range(chips):
        source = lax.rem(chip - step + chips, chips)
        if step > 0:
            back[step].wait_recv()
        last[step] = pltpu.make_async_remote_copy(
            src_ref=out.at[core, source],
            dst_ref=out.at[core, source],
            send_sem=last_send.at[step],
            recv_sem=last_recv.at[step],
            device_id=partner,
            device_id_type=MESH,
        )
        last[step].start()
    for step in range(chips):
        last[step].wait_recv()
    for copies in (pairs, across, along, back, last):
        for copy in copies.values():
            copy.wait_send()


def all_sum(part, planes):
    _, chips, rows, width = part.shape
    dma = pltpu.SemaphoreType.DMA
    vmem = pl.BlockSpec(memory_space=pltpu.VMEM)
    return pl.pallas_call(
        functools.partial(reduce_kernel, chips, planes),
        out_shape=jax.ShapeDtypeStruct(part.shape, jnp.float32),
        in_specs=[vmem],
        out_specs=vmem,
        scratch_shapes=[
            pltpu.VMEM((chips, rows, width), jnp.float32),
            pltpu.VMEM((chips, rows, width), jnp.float32),
            pltpu.VMEM((chips, rows, width), jnp.float32),
            pltpu.VMEM((planes, rows, width), jnp.float32),
        ]
        + [dma((chips,)), dma((chips,)), dma((chips,)), dma((chips,)), dma((planes,)), dma((planes,))]
        + [dma((chips,)), dma((chips,)), dma((chips,)), dma((chips,))],
        compiler_params=pltpu.CompilerParams(collective_id=0, has_side_effects=True),
        name="all_sum",
    )(part)


def shift_rows(value, steps):
    length = value.shape[0]
    row = lax.broadcasted_iota(jnp.int32, value.shape, 0)
    moved = pltpu.roll(value, steps % length, 0)
    keep = row >= steps if steps > 0 else row < length + steps
    return jnp.where(keep, moved, 0.0)


def powers(matrix, count):
    low = [matrix]
    while len(low) < SLABS:
        low = low + [dot_high(low[-1], each) for each in low]
    high = []
    square = low[-1]
    for _ in range(count - 1):
        square = dot_high(square, square)
        high.append(square)
    return [weights(each) for each in low], [weights(low[-1])] + [weights(each) for each in high]


def scan_slabs(slabs, low, high, reverse):
    order = list(range(SLABS))[::-1] if reverse else list(range(SLABS))
    sign = -1 if reverse else 1
    part = {order[0]: slabs[order[0]]}
    for before, now in zip(order, order[1:]):
        part[now] = slabs[now] + times(part[before], low[0])
    ends = part[order[-1]]
    for level, power in enumerate(high):
        ends = ends + times(shift_rows(ends, sign * 2**level), power)
    carry = shift_rows(ends, sign)
    out = [None] * SLABS
    for place, now in enumerate(order[:-1]):
        out[now] = part[now] + times(carry, low[place])
    out[order[-1]] = ends
    return out


def invert(matrices):
    size = matrices[0].shape[0]
    row_at = lax.broadcasted_iota(jnp.int32, (size, size), 0)
    lane_at = lax.broadcasted_iota(jnp.int32, (size, size), 1)
    lane = lax.broadcasted_iota(jnp.int32, (1, size), 1)
    for k in range(size):
        following = []
        for m in matrices:
            column = m[:, k : k + 1]
            row = m[k : k + 1, :]
            scale = 1.0 / m[k : k + 1, k : k + 1]
            row = jnp.where(lane == k, scale, row * scale)
            base = jnp.where(lane_at == k, 0.0, m)
            m = jnp.where(row_at == k, row, base - column * row)
            following.append(m)
        matrices = following
    return matrices


def smooth_kernel(
    length, total_in, transition, filter_cov, gain, cov, smoothed, inverse, moved, drive
):
    width = transition.shape[0]
    _, chips, rows, _ = total_in.shape
    block = length // (2 * chips)
    count = length // SLABS
    levels = (count - 1).bit_length()
    info = jnp.concatenate(
        [total_in[core, chip, block:, :] for chip in range(chips) for core in range(2)], axis=0
    )
    closed = transition[...] - dot_high(filter_cov[...], dot_high(info, transition[...]))
    low, high = powers(closed.T, levels)
    cov_t = weights(filter_cov[...].T)
    for chip in range(chips):
        for core in range(2):
            start = (2 * chip + core) * block
            drive[start : start + block, :] = times(total_in[core, chip, :block, :], cov_t)
    slabs = [drive[pl.ds(at, count, stride=SLABS), :] for at in range(SLABS)]
    filtered = scan_slabs(slabs, low, high, False)
    coupled = weights(dot_high(gain[...], transition[...]).T)
    last = lax.broadcasted_iota(jnp.int32, (count, width), 0) == count - 1
    back = [each - times(each, coupled) for each in filtered]
    back[-1] = jnp.where(last, filtered[-1], back[-1])
    low, high = powers(gain[...].T, levels)
    smooth = scan_slabs(back, low, high, True)
    for at in range(SLABS):
        smoothed[pl.ds(at, count, stride=SLABS), :] = smooth[at]
    kept = smooth[:-1] + [jnp.where(last, 0.0, smooth[-1])]
    previous = sum(dot_first(each, each) for each in kept)
    final = smooth[-1][count - 8 :, :]
    final = jnp.where(lax.broadcasted_iota(jnp.int32, final.shape, 0) == 7, final, 0.0)
    total = previous + dot_first(final, final)
    lag = [shift_rows(smooth[-1], 1)] + smooth[:-1]
    lagged = sum(dot_first(each, before) for each, before in zip(smooth, lag))
    total = total + length * cov[...]
    previous = previous + (length - 1) * cov[...]
    lagged = lagged + (length - 1) * dot_high(cov[...], gain[...].T)
    total, previous = invert([total, previous])
    inverse[...] = total
    moved[...] = dot_high(lagged, previous)


def local(
    observations, loadings, noise_precision, transition, filter_cov, smoother_gain, smoothed_cov
):
    blocks = lax.axis_size("tm")
    planes = lax.axis_size("sr")
    position = lax.axis_index("tm")
    width = transition.shape[0]
    length = observations.shape[0]
    steps_dev = length // blocks
    weighted = noise_precision[:, None] * loadings
    proj = jnp.dot(
        observations, weighted.astype(jnp.bfloat16), preferred_element_type=jnp.float32
    )
    info = dot_high(loadings.T, weighted)
    part = jnp.concatenate(
        [proj.reshape(blocks, steps_dev, width), info.reshape(blocks, width // blocks, width)], axis=1
    )
    part = part.reshape(blocks // 2, 2, part.shape[1], width).transpose(1, 0, 2, 3)
    summed = all_sum(part, planes)
    vmem = pl.BlockSpec(memory_space=pltpu.VMEM)
    smoothed, inverse, new_transition = pl.pallas_call(
        functools.partial(smooth_kernel, length),
        out_shape=[
            jax.ShapeDtypeStruct((length, width), jnp.float32),
            jax.ShapeDtypeStruct((width, width), jnp.float32),
            jax.ShapeDtypeStruct((width, width), jnp.float32),
        ],
        in_specs=[vmem] * 5,
        out_specs=[vmem] * 3,
        scratch_shapes=[pltpu.VMEM((length, width), jnp.float32)],
        name="smooth",
    )(summed, transition, filter_cov, smoother_gain, smoothed_cov)
    cross = jnp.einsum(
        "ts,tk->sk",
        observations,
        smoothed.astype(jnp.bfloat16),
        preferred_element_type=jnp.float32,
    )
    new_loadings = dot_high(cross, inverse)
    own = lax.dynamic_slice_in_dim(smoothed, position * steps_dev, steps_dev, 0)
    return (own, new_loadings, new_transition)


def solution(mesh):
    in_specs = (P(None, ("sr", "tm")), P(("sr", "tm"), None), P(("sr", "tm")), P(), P(), P(), P())
    out_specs = (P("tm", None), P(("sr", "tm"), None), P())
    return jax.shard_map(local, mesh=mesh, in_specs=in_specs, out_specs=out_specs, check_vma=False)
```

```python
import functools
import jax
import jax.numpy as jnp
from jax import lax
from jax.experimental import pallas as pl
from jax.experimental.pallas import tpu as pltpu
from jax.sharding import PartitionSpec as P

precise = lax.Precision.HIGHEST
MESH = pl.DeviceIdType.MESH
SLABS = 8
PIECES = 2
PIVOTS = 4


def dot_high(left, right):
    return jnp.dot(left, right, precision=precise, preferred_element_type=jnp.float32)


def dot_first(left, right):
    return lax.dot_general(
        left, right, (((0,), (0,)), ((), ())), precision=precise, preferred_element_type=jnp.float32
    )


def halves(value):
    high = value.astype(jnp.bfloat16)
    low = (value - high.astype(jnp.float32)).astype(jnp.bfloat16)
    return high, low


def weights(matrix):
    high, low = halves(matrix)
    side = jnp.concatenate([high, low], axis=1)
    return jnp.concatenate([side, side], axis=0)


def times(value, doubled):
    high, low = halves(value)
    width = value.shape[1]
    out = jnp.dot(
        jnp.concatenate([high, low], axis=1), doubled, preferred_element_type=jnp.float32
    )
    return out[:, :width] + out[:, width:]


def project_kernel(observations, loadings, precision, out):
    _, chips, rows, width = out.shape
    block = observations.shape[0] // (2 * chips)
    depth = loadings.shape[0]
    columns = [
        jnp.broadcast_to(precision[pl.ds(at, 1), :], (width, width)).T
        for at in range(depth // width)
    ]
    weighted = loadings[...] * jnp.concatenate(columns, axis=0)
    proj = jnp.dot(
        observations[...], weighted.astype(jnp.bfloat16), preferred_element_type=jnp.float32
    )
    left = jnp.concatenate(halves(loadings[...]), axis=1)
    right = jnp.concatenate(halves(weighted), axis=1)
    both = lax.dot_general(
        left, right, (((0,), (0,)), ((), ())), preferred_element_type=jnp.float32
    )
    both = both[:width] + both[width:]
    info = both[:, :width] + both[:, width:]
    share = width // (2 * chips)

    @pl.when(pl.program_id(0) == 0)
    def _():
        out[...] = jnp.zeros_like(out)

    for chip in range(chips):
        for core in range(2):
            at = 2 * chip + core
            out[core, chip, :block, :] += proj[at * block : (at + 1) * block]
            out[core, chip, block:, :] += info[at * share : (at + 1) * share]


def project(observations, loadings, noise_precision, blocks):
    length, series = observations.shape
    width = loadings.shape[1]
    depth = min(series, 512)
    lanes = depth // width
    shape = (2, blocks // 2, (length + width) // blocks, width)
    return pl.pallas_call(
        project_kernel,
        grid=(series // depth,),
        out_shape=jax.ShapeDtypeStruct(shape, jnp.float32),
        in_specs=[
            pl.BlockSpec((length, depth), lambda at: (0, at)),
            pl.BlockSpec((depth, width), lambda at: (at, 0)),
            pl.BlockSpec((None, lanes, width), lambda at: (at, 0, 0)),
        ],
        out_specs=pl.BlockSpec(shape, lambda at: (0, 0, 0, 0)),
        name="project",
    )(observations, loadings, noise_precision.reshape(series // depth, lanes, width))


def reduce_kernel(
    chips, planes, pieces, part, out, pair_in, mine, chip_in, plane_in,
    pair_send, pair_recv, chip_send, chip_recv, plane_send, plane_recv,
    back_send, back_recv, last_send, last_recv,
):
    tm = lax.axis_index("tm")
    sr = lax.axis_index("sr")
    core = lax.rem(tm, 2)
    chip = tm // 2
    other = 1 - core
    partner = (2 * chip + other, sr)

    def chip_at(step):
        return lax.rem(chip + step, chips)

    def plane_at(step):
        return lax.rem(sr + step, planes)

    barrier = pltpu.get_barrier_semaphore()
    pl.semaphore_signal(barrier, inc=1, device_id=partner, device_id_type=MESH)
    for step in range(1, chips):
        pl.semaphore_signal(
            barrier, inc=1, device_id=(2 * chip_at(step) + core, sr), device_id_type=MESH
        )
    for step in range(1, planes):
        pl.semaphore_signal(barrier, inc=1, device_id=(tm, plane_at(step)), device_id_type=MESH)
    pl.semaphore_wait(barrier, 1 + chips - 1 + planes - 1)

    order = list(range(1, chips)) + [0]
    pairs, across, along, back, last = {}, {}, {}, {}, {}
    for at, rows in enumerate(pieces):
        for step in order:
            target = chip_at(step)
            pairs[at, step] = pltpu.make_async_remote_copy(
                src_ref=part.at[other, target, rows],
                dst_ref=pair_in.at[step, rows],
                send_sem=pair_send.at[at, step],
                recv_sem=pair_recv.at[at, step],
                device_id=partner,
                device_id_type=MESH,
            )
            pairs[at, step].start()
    for at, rows in enumerate(pieces):
        for step in order:
            pairs[at, step].wait_recv()
            mine[step, rows] = part[core, chip_at(step), rows] + pair_in[step, rows]
            if step > 0:
                across[at, step] = pltpu.make_async_remote_copy(
                    src_ref=mine.at[step, rows],
                    dst_ref=chip_in.at[step, rows],
                    send_sem=chip_send.at[at, step],
                    recv_sem=chip_recv.at[at, step],
                    device_id=(2 * chip_at(step) + core, sr),
                    device_id_type=MESH,
                )
                across[at, step].start()
    for at, rows in enumerate(pieces):
        total = mine[0, rows]
        for step in range(1, chips):
            across[at, step].wait_recv()
            total = total + chip_in[step, rows]
        plane_in[sr, rows] = total
        for step in range(1, planes):
            along[at, step] = pltpu.make_async_remote_copy(
                src_ref=plane_in.at[sr, rows],
                dst_ref=plane_in.at[sr, rows],
                send_sem=plane_send.at[at, step],
                recv_sem=plane_recv.at[at, step],
                device_id=(tm, plane_at(step)),
                device_id_type=MESH,
            )
            along[at, step].start()

    def pass_on(at, rows, step):
        source = lax.rem(chip - step + chips, chips)
        last[at, step] = pltpu.make_async_remote_copy(
            src_ref=out.at[core, source, rows],
            dst_ref=out.at[core, source, rows],
            send_sem=last_send.at[at, step],
            recv_sem=last_recv.at[at, step],
            device_id=partner,
            device_id_type=MESH,
        )
        last[at, step].start()

    for at, rows in enumerate(pieces):
        for step in range(1, planes):
            along[at, step].wait_recv()
        whole = plane_in[0, rows]
        for plane in range(1, planes):
            whole = whole + plane_in[plane, rows]
        out[core, chip, rows] = whole
        for step in range(1, chips):
            back[at, step] = pltpu.make_async_remote_copy(
                src_ref=out.at[core, chip, rows],
                dst_ref=out.at[core, chip, rows],
                send_sem=back_send.at[at, step],
                recv_sem=back_recv.at[at, step],
                device_id=(2 * chip_at(step) + core, sr),
                device_id_type=MESH,
            )
            back[at, step].start()
        pass_on(at, rows, 0)
    for at, rows in enumerate(pieces):
        for step in range(1, chips):
            back[at, step].wait_recv()
            pass_on(at, rows, step)
    for copy in last.values():
        copy.wait_recv()
    for copies in (pairs, across, along, back, last):
        for copy in copies.values():
            copy.wait_send()


def all_sum(part, planes):
    _, chips, rows, width = part.shape
    dma = pltpu.SemaphoreType.DMA
    cuts = [rows * at // PIECES // 8 * 8 for at in range(PIECES)] + [rows]
    pieces = [slice(start, stop) for start, stop in zip(cuts, cuts[1:])]
    vmem = pl.BlockSpec(memory_space=pltpu.VMEM)
    return pl.pallas_call(
        functools.partial(reduce_kernel, chips, planes, pieces),
        out_shape=jax.ShapeDtypeStruct(part.shape, jnp.float32),
        in_specs=[vmem],
        out_specs=vmem,
        scratch_shapes=[
            pltpu.VMEM((chips, rows, width), jnp.float32),
            pltpu.VMEM((chips, rows, width), jnp.float32),
            pltpu.VMEM((chips, rows, width), jnp.float32),
            pltpu.VMEM((planes, rows, width), jnp.float32),
        ]
        + [dma((PIECES, chips))] * 4
        + [dma((PIECES, planes))] * 2
        + [dma((PIECES, chips))] * 4,
        compiler_params=pltpu.CompilerParams(collective_id=0, has_side_effects=True),
        name="all_sum",
    )(part)


def shift_rows(value, steps):
    length = value.shape[0]
    row = lax.broadcasted_iota(jnp.int32, value.shape, 0)
    moved = pltpu.roll(value, steps % length, 0)
    keep = row >= steps if steps > 0 else row < length + steps
    return jnp.where(keep, moved, 0.0)


def powers(matrix, count):
    low = [matrix]
    while len(low) < SLABS:
        low = low + [dot_high(low[-1], each) for each in low]
    high = []
    square = low[-1]
    for _ in range(count - 1):
        square = dot_high(square, square)
        high.append(square)
    return [weights(each) for each in low], [weights(low[-1])] + [weights(each) for each in high]


def scan_slabs(slabs, low, high, reverse):
    order = list(range(SLABS))[::-1] if reverse else list(range(SLABS))
    sign = -1 if reverse else 1
    part = {order[0]: slabs[order[0]]}
    for before, now in zip(order, order[1:]):
        part[now] = slabs[now] + times(part[before], low[0])
    ends = part[order[-1]]
    for level, power in enumerate(high):
        ends = ends + times(shift_rows(ends, sign * 2**level), power)
    carry = shift_rows(ends, sign)
    out = [None] * SLABS
    for place, now in enumerate(order[:-1]):
        out[now] = part[now] + times(carry, low[place])
    out[order[-1]] = ends
    return out


def inverse_two(a, b, c):
    scale = 1.0 / (a * c - b * b)
    return c * scale, -b * scale, a * scale


def inverse_four(p):
    e, f, g = inverse_two(p[0][0], p[0][1], p[1][1])
    u00 = e * p[0][2] + f * p[1][2]
    u01 = e * p[0][3] + f * p[1][3]
    u10 = f * p[0][2] + g * p[1][2]
    u11 = f * p[0][3] + g * p[1][3]
    s00 = p[2][2] - (p[0][2] * u00 + p[1][2] * u10)
    s01 = p[2][3] - (p[0][2] * u01 + p[1][2] * u11)
    s11 = p[3][3] - (p[0][3] * u01 + p[1][3] * u11)
    t00, t01, t11 = inverse_two(s00, s01, s11)
    v00 = u00 * t00 + u01 * t01
    v01 = u00 * t01 + u01 * t11
    v10 = u10 * t00 + u11 * t01
    v11 = u10 * t01 + u11 * t11
    a00 = e + (v00 * u00 + v01 * u01)
    a01 = f + (v00 * u10 + v01 * u11)
    a11 = g + (v10 * u10 + v11 * u11)
    return [
        [a00, a01, -v00, -v01],
        [a01, a11, -v10, -v11],
        [-v00, -v10, t00, t01],
        [-v01, -v11, t01, t11],
    ]


def invert(matrices):
    size = matrices[0].shape[0]
    row_at = lax.broadcasted_iota(jnp.int32, (size, size), 0)
    lane_at = lax.broadcasted_iota(jnp.int32, (size, size), 1)
    lane = lax.broadcasted_iota(jnp.int32, (8, size), 1)
    diagonal = row_at == lane_at
    scales, scaled = [], []
    for m in matrices:
        only = jnp.where(diagonal, m, 0.0)
        across = lax.rsqrt(jnp.sum(only, axis=0, keepdims=True))
        down = lax.rsqrt(jnp.sum(only, axis=1, keepdims=True))
        scales.append((across, down))
        scaled.append((m * across) * down)
    matrices = scaled
    for k in range(0, size, PIVOTS):
        following = []
        group = k // 8 * 8
        for m in matrices:
            columns = [jnp.broadcast_to(m[:, k + j : k + j + 1], m.shape) for j in range(PIVOTS)]

            def spread(value, at):
                return jnp.broadcast_to(value[at : at + 1, :], (8, size))

            block = [
                [spread(columns[j], k + min(i, j)) if i <= j else None for j in range(PIVOTS)]
                for i in range(PIVOTS)
            ]
            rows = [spread(m, k + i) for i in range(PIVOTS)]
            solved = inverse_four(block)
            fresh = []
            for i in range(PIVOTS):
                row = solved[i][0] * rows[0]
                for j in range(1, PIVOTS):
                    row = row + solved[i][j] * rows[j]
                for j in range(PIVOTS):
                    row = jnp.where(lane == k + j, solved[i][j], row)
                fresh.append(row)
            parts = []
            for start in range(0, size, 8):
                here = slice(start, start + 8)
                value = jnp.where((lane >= k) & (lane < k + PIVOTS), 0.0, m[here])
                take = columns[0][here] * fresh[0]
                for i in range(1, PIVOTS):
                    take = take + columns[i][here] * fresh[i]
                value = value - take
                if start == group:
                    for i in range(PIVOTS):
                        value = jnp.where(row_at[here] == k + i, fresh[i], value)
                parts.append(value)
            following.append(jnp.concatenate(parts, axis=0))
        matrices = following
    return [(m * across) * down for m, (across, down) in zip(matrices, scales)]


def smooth_kernel(
    length, total_in, transition, filter_cov, gain, cov, smoothed, inverse, moved, drive
):
    width = transition.shape[0]
    _, chips, rows, _ = total_in.shape
    block = length // (2 * chips)
    count = length // SLABS
    levels = (count - 1).bit_length()
    info = jnp.concatenate(
        [total_in[core, chip, block:, :] for chip in range(chips) for core in range(2)], axis=0
    )
    closed = transition[...] - dot_high(filter_cov[...], dot_high(info, transition[...]))
    low, high = powers(closed.T, levels)
    cov_t = weights(filter_cov[...].T)
    for chip in range(chips):
        for core in range(2):
            start = (2 * chip + core) * block
            drive[start : start + block, :] = times(total_in[core, chip, :block, :], cov_t)
    slabs = [drive[pl.ds(at, count, stride=SLABS), :] for at in range(SLABS)]
    filtered = scan_slabs(slabs, low, high, False)
    coupled = weights(dot_high(gain[...], transition[...]).T)
    last = lax.broadcasted_iota(jnp.int32, (count, width), 0) == count - 1
    back = [each - times(each, coupled) for each in filtered]
    back[-1] = jnp.where(last, filtered[-1], back[-1])
    low, high = powers(gain[...].T, levels)
    smooth = scan_slabs(back, low, high, True)
    for at in range(SLABS):
        smoothed[pl.ds(at, count, stride=SLABS), :] = smooth[at]
    kept = smooth[:-1] + [jnp.where(last, 0.0, smooth[-1])]
    previous = sum(dot_first(each, each) for each in kept)
    final = smooth[-1][count - 8 :, :]
    final = jnp.where(lax.broadcasted_iota(jnp.int32, final.shape, 0) == 7, final, 0.0)
    total = previous + dot_first(final, final)
    lag = [shift_rows(smooth[-1], 1)] + smooth[:-1]
    lagged = sum(dot_first(each, before) for each, before in zip(smooth, lag))
    total = total + length * cov[...]
    previous = previous + (length - 1) * cov[...]
    lagged = lagged + (length - 1) * dot_high(cov[...], gain[...].T)
    total, previous = invert([total, previous])
    inverse[...] = total
    moved[...] = dot_high(lagged, previous)


def local(
    observations, loadings, noise_precision, transition, filter_cov, smoother_gain, smoothed_cov
):
    blocks = lax.axis_size("tm")
    planes = lax.axis_size("sr")
    position = lax.axis_index("tm")
    width = transition.shape[0]
    length = observations.shape[0]
    steps_dev = length // blocks
    part = project(observations, loadings, noise_precision, blocks)
    summed = all_sum(part, planes)
    vmem = pl.BlockSpec(memory_space=pltpu.VMEM)
    smoothed, inverse, new_transition = pl.pallas_call(
        functools.partial(smooth_kernel, length),
        out_shape=[
            jax.ShapeDtypeStruct((length, width), jnp.float32),
            jax.ShapeDtypeStruct((width, width), jnp.float32),
            jax.ShapeDtypeStruct((width, width), jnp.float32),
        ],
        in_specs=[vmem] * 5,
        out_specs=[vmem] * 3,
        scratch_shapes=[pltpu.VMEM((length, width), jnp.float32)],
        name="smooth",
    )(summed, transition, filter_cov, smoother_gain, smoothed_cov)
    cross = jnp.einsum(
        "ts,tk->sk",
        observations,
        smoothed.astype(jnp.bfloat16),
        preferred_element_type=jnp.float32,
    )
    new_loadings = dot_high(cross, inverse)
    own = lax.dynamic_slice_in_dim(smoothed, position * steps_dev, steps_dev, 0)
    return (own, new_loadings, new_transition)


def solution(mesh):
    in_specs = (P(None, ("sr", "tm")), P(("sr", "tm"), None), P(("sr", "tm")), P(), P(), P(), P())
    out_specs = (P("tm", None), P(("sr", "tm"), None), P())
    return jax.shard_map(local, mesh=mesh, in_specs=in_specs, out_specs=out_specs, check_vma=False)
```

```python
import functools
import jax
import jax.numpy as jnp
from jax import lax
from jax.experimental import pallas as pl
from jax.experimental.pallas import tpu as pltpu
from jax.sharding import PartitionSpec as P

precise = lax.Precision.HIGHEST
MESH = pl.DeviceIdType.MESH
SLABS = 8
PIECES = 2
PIVOTS = 4


def dot_high(left, right):
    return jnp.dot(left, right, precision=precise, preferred_element_type=jnp.float32)


def dot_first(left, right):
    return lax.dot_general(
        left, right, (((0,), (0,)), ((), ())), precision=precise, preferred_element_type=jnp.float32
    )


def halves(value):
    high = value.astype(jnp.bfloat16)
    low = (value - high.astype(jnp.float32)).astype(jnp.bfloat16)
    return high, low


def weights(matrix):
    high, low = halves(matrix)
    side = jnp.concatenate([high, low], axis=1)
    return jnp.concatenate([side, side], axis=0)


def times(value, doubled):
    high, low = halves(value)
    width = value.shape[1]
    out = jnp.dot(
        jnp.concatenate([high, low], axis=1), doubled, preferred_element_type=jnp.float32
    )
    return out[:, :width] + out[:, width:]


def project_kernel(observations, loadings, precision, out):
    _, chips, rows, width = out.shape
    block = observations.shape[0] // (2 * chips)
    depth = loadings.shape[0]
    columns = [
        jnp.broadcast_to(precision[pl.ds(at, 1), :], (width, width)).T
        for at in range(depth // width)
    ]
    weighted = loadings[...] * jnp.concatenate(columns, axis=0)
    proj = jnp.dot(
        observations[...], weighted.astype(jnp.bfloat16), preferred_element_type=jnp.float32
    )
    left = jnp.concatenate(halves(loadings[...]), axis=1)
    right = jnp.concatenate(halves(weighted), axis=1)
    both = lax.dot_general(
        left, right, (((0,), (0,)), ((), ())), preferred_element_type=jnp.float32
    )
    both = both[:width] + both[width:]
    info = both[:, :width] + both[:, width:]
    share = width // (2 * chips)

    @pl.when(pl.program_id(0) == 0)
    def _():
        out[...] = jnp.zeros_like(out)

    for chip in range(chips):
        for core in range(2):
            at = 2 * chip + core
            out[core, chip, :block, :] += proj[at * block : (at + 1) * block]
            out[core, chip, block:, :] += info[at * share : (at + 1) * share]


def project(observations, loadings, noise_precision, blocks):
    length, series = observations.shape
    width = loadings.shape[1]
    depth = min(series, 512)
    lanes = depth // width
    shape = (2, blocks // 2, (length + width) // blocks, width)
    return pl.pallas_call(
        project_kernel,
        grid=(series // depth,),
        out_shape=jax.ShapeDtypeStruct(shape, jnp.float32),
        in_specs=[
            pl.BlockSpec((length, depth), lambda at: (0, at)),
            pl.BlockSpec((depth, width), lambda at: (at, 0)),
            pl.BlockSpec((None, lanes, width), lambda at: (at, 0, 0)),
        ],
        out_specs=pl.BlockSpec(shape, lambda at: (0, 0, 0, 0)),
        name="project",
    )(observations, loadings, noise_precision.reshape(series // depth, lanes, width))


def reduce_kernel(
    chips, planes, pieces, part, out, pair_in, mine, chip_in, plane_in,
    pair_send, pair_recv, chip_send, chip_recv, plane_send, plane_recv,
    back_send, back_recv, last_send, last_recv,
):
    tm = lax.axis_index("tm")
    sr = lax.axis_index("sr")
    core = lax.rem(tm, 2)
    chip = tm // 2
    other = 1 - core
    partner = (2 * chip + other, sr)

    def chip_at(step):
        return lax.rem(chip + step, chips)

    def plane_at(step):
        return lax.rem(sr + step, planes)

    barrier = pltpu.get_barrier_semaphore()
    pl.semaphore_signal(barrier, inc=1, device_id=partner, device_id_type=MESH)
    for step in range(1, chips):
        pl.semaphore_signal(
            barrier, inc=1, device_id=(2 * chip_at(step) + core, sr), device_id_type=MESH
        )
    for step in range(1, planes):
        pl.semaphore_signal(barrier, inc=1, device_id=(tm, plane_at(step)), device_id_type=MESH)
    pl.semaphore_wait(barrier, 1 + chips - 1 + planes - 1)

    order = list(range(1, chips)) + [0]
    pairs, across, along, back, last = {}, {}, {}, {}, {}
    for at, rows in enumerate(pieces):
        for step in order:
            target = chip_at(step)
            pairs[at, step] = pltpu.make_async_remote_copy(
                src_ref=part.at[other, target, rows],
                dst_ref=pair_in.at[step, rows],
                send_sem=pair_send.at[at, step],
                recv_sem=pair_recv.at[at, step],
                device_id=partner,
                device_id_type=MESH,
            )
            pairs[at, step].start()
    for at, rows in enumerate(pieces):
        for step in order:
            pairs[at, step].wait_recv()
            mine[step, rows] = part[core, chip_at(step), rows] + pair_in[step, rows]
            if step > 0:
                across[at, step] = pltpu.make_async_remote_copy(
                    src_ref=mine.at[step, rows],
                    dst_ref=chip_in.at[step, rows],
                    send_sem=chip_send.at[at, step],
                    recv_sem=chip_recv.at[at, step],
                    device_id=(2 * chip_at(step) + core, sr),
                    device_id_type=MESH,
                )
                across[at, step].start()
    for at, rows in enumerate(pieces):
        total = mine[0, rows]
        for step in range(1, chips):
            across[at, step].wait_recv()
            total = total + chip_in[step, rows]
        plane_in[sr, rows] = total
        for step in range(1, planes):
            along[at, step] = pltpu.make_async_remote_copy(
                src_ref=plane_in.at[sr, rows],
                dst_ref=plane_in.at[sr, rows],
                send_sem=plane_send.at[at, step],
                recv_sem=plane_recv.at[at, step],
                device_id=(tm, plane_at(step)),
                device_id_type=MESH,
            )
            along[at, step].start()

    def pass_on(at, rows, step):
        source = lax.rem(chip - step + chips, chips)
        last[at, step] = pltpu.make_async_remote_copy(
            src_ref=out.at[core, source, rows],
            dst_ref=out.at[core, source, rows],
            send_sem=last_send.at[at, step],
            recv_sem=last_recv.at[at, step],
            device_id=partner,
            device_id_type=MESH,
        )
        last[at, step].start()

    for at, rows in enumerate(pieces):
        for step in range(1, planes):
            along[at, step].wait_recv()
        whole = plane_in[0, rows]
        for plane in range(1, planes):
            whole = whole + plane_in[plane, rows]
        out[core, chip, rows] = whole
        for step in range(1, chips):
            back[at, step] = pltpu.make_async_remote_copy(
                src_ref=out.at[core, chip, rows],
                dst_ref=out.at[core, chip, rows],
                send_sem=back_send.at[at, step],
                recv_sem=back_recv.at[at, step],
                device_id=(2 * chip_at(step) + core, sr),
                device_id_type=MESH,
            )
            back[at, step].start()
        pass_on(at, rows, 0)
    for at, rows in enumerate(pieces):
        for step in range(1, chips):
            back[at, step].wait_recv()
            pass_on(at, rows, step)
    for copy in last.values():
        copy.wait_recv()
    for copies in (pairs, across, along, back, last):
        for copy in copies.values():
            copy.wait_send()


def all_sum(part, planes):
    _, chips, rows, width = part.shape
    dma = pltpu.SemaphoreType.DMA
    cuts = [rows * at // PIECES // 8 * 8 for at in range(PIECES)] + [rows]
    pieces = [slice(start, stop) for start, stop in zip(cuts, cuts[1:])]
    vmem = pl.BlockSpec(memory_space=pltpu.VMEM)
    return pl.pallas_call(
        functools.partial(reduce_kernel, chips, planes, pieces),
        out_shape=jax.ShapeDtypeStruct(part.shape, jnp.float32),
        in_specs=[vmem],
        out_specs=vmem,
        scratch_shapes=[
            pltpu.VMEM((chips, rows, width), jnp.float32),
            pltpu.VMEM((chips, rows, width), jnp.float32),
            pltpu.VMEM((chips, rows, width), jnp.float32),
            pltpu.VMEM((planes, rows, width), jnp.float32),
        ]
        + [dma((PIECES, chips))] * 4
        + [dma((PIECES, planes))] * 2
        + [dma((PIECES, chips))] * 4,
        compiler_params=pltpu.CompilerParams(collective_id=0, has_side_effects=True),
        name="all_sum",
    )(part)


def shift_rows(value, steps):
    length = value.shape[0]
    row = lax.broadcasted_iota(jnp.int32, value.shape, 0)
    moved = pltpu.roll(value, steps % length, 0)
    keep = row >= steps if steps > 0 else row < length + steps
    return jnp.where(keep, moved, 0.0)


def powers(matrix, count):
    low = [matrix]
    while len(low) < SLABS:
        low = low + [dot_high(low[-1], each) for each in low]
    high = []
    square = low[-1]
    for _ in range(count - 1):
        square = dot_high(square, square)
        high.append(square)
    return [weights(each) for each in low], [weights(low[-1])] + [weights(each) for each in high]


def scan_slabs(slabs, low, high, reverse):
    order = list(range(SLABS))[::-1] if reverse else list(range(SLABS))
    sign = -1 if reverse else 1
    part = {order[0]: slabs[order[0]]}
    for before, now in zip(order, order[1:]):
        part[now] = slabs[now] + times(part[before], low[0])
    ends = part[order[-1]]
    for level, power in enumerate(high):
        ends = ends + times(shift_rows(ends, sign * 2**level), power)
    carry = shift_rows(ends, sign)
    out = [None] * SLABS
    for place, now in enumerate(order[:-1]):
        out[now] = part[now] + times(carry, low[place])
    out[order[-1]] = ends
    return out


def inverse_two(a, b, c):
    scale = 1.0 / (a * c - b * b)
    return c * scale, -b * scale, a * scale


def inverse_four(p):
    e, f, g = inverse_two(p[0][0], p[0][1], p[1][1])
    u00 = e * p[0][2] + f * p[1][2]
    u01 = e * p[0][3] + f * p[1][3]
    u10 = f * p[0][2] + g * p[1][2]
    u11 = f * p[0][3] + g * p[1][3]
    s00 = p[2][2] - (p[0][2] * u00 + p[1][2] * u10)
    s01 = p[2][3] - (p[0][2] * u01 + p[1][2] * u11)
    s11 = p[3][3] - (p[0][3] * u01 + p[1][3] * u11)
    t00, t01, t11 = inverse_two(s00, s01, s11)
    v00 = u00 * t00 + u01 * t01
    v01 = u00 * t01 + u01 * t11
    v10 = u10 * t00 + u11 * t01
    v11 = u10 * t01 + u11 * t11
    a00 = e + (v00 * u00 + v01 * u01)
    a01 = f + (v00 * u10 + v01 * u11)
    a11 = g + (v10 * u10 + v11 * u11)
    return [
        [a00, a01, -v00, -v01],
        [a01, a11, -v10, -v11],
        [-v00, -v10, t00, t01],
        [-v01, -v11, t01, t11],
    ]


def invert(matrices):
    size = matrices[0].shape[0]
    row_at = lax.broadcasted_iota(jnp.int32, (size, size), 0)
    lane_at = lax.broadcasted_iota(jnp.int32, (size, size), 1)
    lane = lax.broadcasted_iota(jnp.int32, (8, size), 1)
    diagonal = row_at == lane_at
    scales, scaled = [], []
    for m in matrices:
        only = jnp.where(diagonal, m, 0.0)
        across = lax.rsqrt(jnp.sum(only, axis=0, keepdims=True))
        down = lax.rsqrt(jnp.sum(only, axis=1, keepdims=True))
        scales.append((across, down))
        scaled.append((m * across) * down)
    matrices = scaled
    for k in range(0, size, PIVOTS):
        following = []
        group = k // 8 * 8
        for m in matrices:
            columns = [jnp.broadcast_to(m[:, k + j : k + j + 1], m.shape) for j in range(PIVOTS)]

            def spread(value, at):
                return jnp.broadcast_to(value[at : at + 1, :], (8, size))

            block = [
                [spread(columns[j], k + min(i, j)) if i <= j else None for j in range(PIVOTS)]
                for i in range(PIVOTS)
            ]
            rows = [spread(m, k + i) for i in range(PIVOTS)]
            solved = inverse_four(block)
            fresh = []
            for i in range(PIVOTS):
                row = solved[i][0] * rows[0]
                for j in range(1, PIVOTS):
                    row = row + solved[i][j] * rows[j]
                for j in range(PIVOTS):
                    row = jnp.where(lane == k + j, solved[i][j], row)
                fresh.append(row)
            parts = []
            for start in range(0, size, 8):
                here = slice(start, start + 8)
                value = jnp.where((lane >= k) & (lane < k + PIVOTS), 0.0, m[here])
                take = columns[0][here] * fresh[0]
                for i in range(1, PIVOTS):
                    take = take + columns[i][here] * fresh[i]
                value = value - take
                if start == group:
                    for i in range(PIVOTS):
                        value = jnp.where(row_at[here] == k + i, fresh[i], value)
                parts.append(value)
            following.append(jnp.concatenate(parts, axis=0))
        matrices = following
    return [(m * across) * down for m, (across, down) in zip(matrices, scales)]


def smooth_kernel(
    total_in, transition, filter_cov, gain, cov, observations, own, updated, moved,
    drive, held, arrived,
):
    length = observations.shape[0]
    panel = pltpu.make_async_copy(observations, held, arrived)
    panel.start()
    width = transition.shape[0]
    _, chips, rows, _ = total_in.shape
    block = length // (2 * chips)
    count = length // SLABS
    levels = (count - 1).bit_length()
    info = jnp.concatenate(
        [total_in[core, chip, block:, :] for chip in range(chips) for core in range(2)], axis=0
    )
    closed = transition[...] - dot_high(filter_cov[...], dot_high(info, transition[...]))
    low, high = powers(closed.T, levels)
    cov_t = weights(filter_cov[...].T)
    for chip in range(chips):
        for core in range(2):
            start = (2 * chip + core) * block
            drive[start : start + block, :] = times(total_in[core, chip, :block, :], cov_t)
    slabs = [drive[pl.ds(at, count, stride=SLABS), :] for at in range(SLABS)]
    filtered = scan_slabs(slabs, low, high, False)
    coupled = weights(dot_high(gain[...], transition[...]).T)
    last = lax.broadcasted_iota(jnp.int32, (count, width), 0) == count - 1
    back = [each - times(each, coupled) for each in filtered]
    back[-1] = jnp.where(last, filtered[-1], back[-1])
    low, high = powers(gain[...].T, levels)
    smooth = scan_slabs(back, low, high, True)
    for at in range(SLABS):
        drive[pl.ds(at, count, stride=SLABS), :] = smooth[at]
    place = pl.multiple_of(lax.axis_index("tm") * block, block)
    own[...] = drive[pl.ds(place, block), :]
    kept = smooth[:-1] + [jnp.where(last, 0.0, smooth[-1])]
    previous = sum(dot_first(each, each) for each in kept)
    final = smooth[-1][count - 8 :, :]
    final = jnp.where(lax.broadcasted_iota(jnp.int32, final.shape, 0) == 7, final, 0.0)
    total = previous + dot_first(final, final)
    lag = [shift_rows(smooth[-1], 1)] + smooth[:-1]
    lagged = sum(dot_first(each, before) for each, before in zip(smooth, lag))
    total = total + length * cov[...]
    previous = previous + (length - 1) * cov[...]
    lagged = lagged + (length - 1) * dot_high(cov[...], gain[...].T)
    factors = drive[...].T.astype(jnp.bfloat16)
    panel.wait()
    series = updated.shape[0]
    parts = [slice(start, min(start + 256, series)) for start in range(0, series, 256)]
    for part in parts:
        updated[part, :] = jnp.dot(
            factors, held[:, part], preferred_element_type=jnp.float32
        ).T
    total, previous = invert([total, previous])
    total = weights(total)
    for part in parts:
        updated[part, :] = times(updated[part, :], total)
    moved[...] = dot_high(lagged, previous)


def local(
    observations, loadings, noise_precision, transition, filter_cov, smoother_gain, smoothed_cov
):
    blocks = lax.axis_size("tm")
    planes = lax.axis_size("sr")
    width = transition.shape[0]
    length = observations.shape[0]
    steps_dev = length // blocks
    part = project(observations, loadings, noise_precision, blocks)
    summed = all_sum(part, planes)
    vmem = pl.BlockSpec(memory_space=pltpu.VMEM)
    series = observations.shape[1]
    return pl.pallas_call(
        smooth_kernel,
        out_shape=[
            jax.ShapeDtypeStruct((steps_dev, width), jnp.float32),
            jax.ShapeDtypeStruct((series, width), jnp.float32),
            jax.ShapeDtypeStruct((width, width), jnp.float32),
        ],
        in_specs=[vmem] * 5 + [pl.BlockSpec(memory_space=pl.ANY)],
        out_specs=[vmem] * 3,
        scratch_shapes=[
            pltpu.VMEM((length, width), jnp.float32),
            pltpu.VMEM((length, series), observations.dtype),
            pltpu.SemaphoreType.DMA,
        ],
        name="smooth",
    )(summed, transition, filter_cov, smoother_gain, smoothed_cov, observations)


def solution(mesh):
    in_specs = (P(None, ("sr", "tm")), P(("sr", "tm"), None), P(("sr", "tm")), P(), P(), P(), P())
    out_specs = (P("tm", None), P(("sr", "tm"), None), P())
    return jax.shard_map(local, mesh=mesh, in_specs=in_specs, out_specs=out_specs, check_vma=False)
```
